32 devices in a mesh: dp: 4 (over y, x), shard: 8 (over z, core).
Axes of the slice: x: 2, y: 2, z: 4, core: 2. Of those that a mesh axis runs over, the one named last changes fastest.
Arguments:
- gradients: bfloat16 [4, 1536, 2048], P('dp', 'shard'), may hold values from -4000 to 4000, as said below
- master_weights: float32 [1536, 2048], P(('shard', 'dp')), may hold values from -6 to 6
- first_moment: float32 [1536, 2048], P(('shard', 'dp')), may hold values from -4 to 4
- second_moment: float32 [1536, 2048], P(('shard', 'dp')), may hold values from 0.05 to 2
Outputs:
- parameters: bfloat16 [1536, 2048], P('shard')
- new_master: float32 [1536, 2048], P(('shard', 'dp'))
- new_first: float32 [1536, 2048], P(('shard', 'dp'))
- new_second: float32 [1536, 2048], P(('shard', 'dp'))
The draws below stay inside these ranges and needn't reach their ends.
Inputs may be any that keep to these rules, and one draw needn't show every extreme that they name: `gradients`: each replica's partial gradient.
All inputs are finite; a program needn't handle non-finite values.
Results may differ from the reference program's by a relative error of at most 0.006.
Values may be sent and summed in bfloat16 or wider, within the bound.
A program may use at most 64 MiB of HBM per device.

```python
import math
import jax
import jax.numpy as jnp
from jax import lax

D = 2048
ROWS_DEV = 48
ROWS = 1536
N_DP = 4


def draw_gradients(key, part):
    keys = jax.random.split(jax.random.fold_in(key, 17), 7)
    shape = (N_DP, ROWS, D)
    groups = ROWS // ROWS_DEV
    group_of_row = jnp.arange(ROWS, dtype=jnp.int32) // ROWS_DEV
    common = jnp.clip(jax.random.normal(keys[5], (1, ROWS, D), jnp.float32), -5.0, 5.0)
    independent = jnp.clip(jax.random.normal(keys[0], shape, jnp.float32), -5.0, 5.0)
    agreement = jax.random.uniform(keys[4], (groups,), jnp.float32, -1.0, 2.0)
    base = independent + agreement[group_of_row][None, :, None] * common
    rise = jnp.arange(ROWS, dtype=jnp.float32) / max(ROWS - 1, 1)
    row_scale = jnp.exp(jax.random.uniform(keys[1], (ROWS,), jnp.float32) * math.log(10.0)) * jnp.exp(rise * math.log(3.0))
    col_scale = jnp.exp(jax.random.uniform(keys[2], (D,), jnp.float32) * math.log(10.0))
    group_keys = jax.random.split(keys[3], groups)
    order = jax.vmap(lambda one_key: jax.random.permutation(one_key, N_DP))(group_keys).astype(jnp.float32)
    rep_table = jnp.exp(order / max(N_DP - 1, 1) * math.log(3.0)) * jnp.exp(jax.random.uniform(keys[6], (groups, N_DP), jnp.float32) * 0.4)
    rep_scale = jnp.transpose(rep_table[group_of_row])
    values = base * row_scale[None, :, None] * col_scale[None, None, :] * rep_scale[:, :, None] * 0.1
    return values.astype(jnp.bfloat16)


def steps_of(own_key, shape, shards, least, top_value):
    level, own = 1.0, jax.random.fold_in(own_key, 6)
    for axis_at, blocks in shards:
        heights = jnp.exp(jax.random.uniform(jax.random.fold_in(own, axis_at), (blocks,), jnp.float32, least / len(shards), top_value / len(shards)))
        level = level * jnp.repeat(heights, shape[axis_at] // blocks).reshape([-1 if axis == axis_at else 1 for axis in range(len(shape))])
    return level


def centred(own_key, dims, scale, bound, shards=(), kind=jnp.bfloat16):
    gain = steps_of(own_key, dims, shards, -0.22, 0.18) if shards else 1.0
    drawn = jax.random.normal(own_key, dims, jnp.float32) * scale * gain
    return jnp.minimum(jnp.maximum(drawn, -bound), bound).astype(kind)


def setup_inputs(seed: int = 0) -> dict:
    key_list = jax.random.split(jax.random.key(seed), 5)
    gradients = draw_gradients(jax.random.fold_in(key_list[4], 71), 0)
    master_weights = centred(key_list[1], (ROWS, D), 1.0, 6.0, ((0, 32),), jnp.float32)
    first_moment = centred(key_list[2], (ROWS, D), 0.3, 4.0, ((0, 32),), jnp.float32)
    second_moment = jnp.clip(jnp.exp(math.log(2.0) - 3.6888794 * jax.random.uniform(key_list[3], (ROWS, D), jnp.float32) ** steps_of(key_list[3], (ROWS, D), ((0, 32),), -0.2, 0.2)), 0.05, 2.0)
    return dict(gradients=gradients, master_weights=master_weights, first_moment=first_moment, second_moment=second_moment)


first_bias = 1.0 - math.exp(100.0 * math.log(0.9))
second_bias = 1.0 - math.exp(100.0 * math.log(0.95))

def adam_update(summed, factor, master_weights, first_moment, second_moment):
    clipped = factor * summed
    new_first = 0.9 * first_moment + 0.1 * clipped
    new_second = 0.95 * second_moment + 0.05 * clipped * clipped
    first_hat = new_first / first_bias
    second_hat = new_second / second_bias
    new_master = master_weights - 0.01 * (first_hat / (jnp.sqrt(second_hat) + 1e-08) + 0.1 * master_weights)
    return (new_master, new_first, new_second)

def reference(gradients, master_weights, first_moment, second_moment):

    def accumulate(total, piece):
        return (total + piece.astype(jnp.float32), None)
    summed, unused = lax.scan(accumulate, jnp.zeros(gradients.shape[1:], jnp.float32), gradients)
    square_sum = jnp.sum(summed * summed)
    limit = 0.5 * math.sqrt(ROWS * D)
    factor = jnp.minimum(1.0, limit / jnp.sqrt(square_sum + 1e-06))
    new_master, new_first, new_second = adam_update(summed, factor, master_weights, first_moment, second_moment)
    parameters = new_master.astype(jnp.bfloat16)
    return (parameters, new_master, new_first, new_second)
```

```python
import functools
import math

import jax
import jax.numpy as jnp
from jax import lax
from jax.experimental import pallas as pl
from jax.experimental.pallas import tpu as pltpu
from jax.sharding import PartitionSpec as P

MESH = pl.DeviceIdType.MESH
first_bias = 1.0 - math.exp(100.0 * math.log(0.9))
second_bias = 1.0 - math.exp(100.0 * math.log(0.95))


def grid_of(n_dp):
    ny = max(d for d in range(1, math.isqrt(n_dp) + 1) if n_dp % d == 0)
    return ny, n_dp // ny


def copies_of(ny, nx, n_sh):
    return 4 * ny * nx + 2 * (ny + nx) + ny * nx + n_sh


def step_kernel(
    ny, nx, n_sh, entries,
    g, w, m, v,
    out_p, out_w, out_m, out_v,
    gv, wv, mv, vv, sv, pv,
    r1a, r1b, s2a, s2b, r2a, r2b, fa, fb,
    d_own, d_in, h_own, h_in,
    lsem, ssem, rsem,
):
    n_dp = ny * nx
    rows, width = w.shape
    half = width // 2
    tile_r = 16 if rows % 16 == 0 else rows
    tile_c = 512 if half % 512 == 0 else half
    me = lax.axis_index("dp")
    sh = lax.axis_index("shard")
    y, x = me // nx, lax.rem(me, nx)
    count = [0]
    local_count = [0]
    started = []
    local_started = []

    def at_y(k):
        return lax.rem(y + k, ny)

    def at_x(j):
        return lax.rem(x + j, nx)

    def block(by, bx):
        return pl.ds(pl.multiple_of((by * nx + bx) * rows, rows), rows)

    def send(src, dst, target):
        i = count[0]
        count[0] += 1
        copy = pltpu.make_async_remote_copy(
            src_ref=src, dst_ref=dst, send_sem=ssem.at[i], recv_sem=rsem.at[i],
            device_id=target, device_id_type=MESH,
        )
        copy.start()
        started.append(copy)
        return copy

    def local(src, dst):
        i = local_count[0]
        local_count[0] += 1
        copy = pltpu.make_async_copy(src, dst, lsem.at[i])
        copy.start()
        return copy

    barrier = pltpu.get_barrier_semaphore()
    for i in range(1, n_dp):
        pl.semaphore_signal(
            barrier, inc=1, device_id={"dp": lax.rem(me + i, n_dp)}, device_id_type=MESH
        )
    for i in range(1, n_sh):
        pl.semaphore_signal(
            barrier, inc=1, device_id={"shard": lax.rem(sh + i, n_sh)}, device_id_type=MESH
        )
    grads_in = local(g.at[0], gv)
    state_in = [local(w, wv), local(m, mv), local(v, vv)]
    grads_in.wait()
    pl.semaphore_wait(barrier, n_dp - 1 + n_sh - 1)

    cols_a, cols_b = pl.ds(0, half), pl.ds(half, half)

    first_a, first_b = {}, {}
    for j in list(range(1, nx)) + [0]:
        for k in range(1, ny):
            first_a[k, j] = send(
                gv.at[block(at_y(k), at_x(j)), cols_a], r1a.at[k - 1, j],
                {"dp": at_y(k) * nx + x},
            )
    for k in list(range(1, ny)) + [0]:
        for j in range(1, nx):
            first_b[j, k] = send(
                gv.at[block(at_y(k), at_x(j)), cols_b], r1b.at[j - 1, k],
                {"dp": y * nx + at_x(j)},
            )

    def tiles():
        for r in range(0, rows, tile_r):
            for c in range(0, half, tile_c):
                yield r, c

    def own_rows(by, bx, r):
        start = pl.multiple_of((by * nx + bx) * rows + r, tile_r)
        return pl.ds(start, tile_r)

    second_a, second_b = [], []
    for j in range(1, nx):
        for k in range(1, ny):
            first_a[k, j].wait_recv()
        for r, c in tiles():
            here = (pl.ds(r, tile_r), pl.ds(c, tile_c))
            part = gv[own_rows(y, at_x(j), r), pl.ds(c, tile_c)].astype(jnp.float32)
            for k in range(1, ny):
                part = part + r1a[(k - 1, j) + here].astype(jnp.float32)
            s2a[(j - 1,) + here] = part.astype(jnp.bfloat16)
        second_a.append(send(s2a.at[j - 1], r2a.at[j - 1], {"dp": y * nx + at_x(j)}))
    for k in range(1, ny):
        for j in range(1, nx):
            first_b[j, k].wait_recv()
        for r, c in tiles():
            here = (pl.ds(r, tile_r), pl.ds(c, tile_c))
            part = gv[own_rows(at_y(k), x, r), pl.ds(half + c, tile_c)].astype(jnp.float32)
            for j in range(1, nx):
                part = part + r1b[(j - 1, k) + here].astype(jnp.float32)
            s2b[(k - 1,) + here] = part.astype(jnp.bfloat16)
        second_b.append(send(s2b.at[k - 1], r2b.at[k - 1], {"dp": at_y(k) * nx + x}))

    for k in range(1, ny):
        first_a[k, 0].wait_recv()
    for j in range(1, nx):
        first_b[j, 0].wait_recv()
    squares = jnp.zeros((8, 128), jnp.float32)
    for base, first, first_n, second, later in (
        (0, r1a, ny - 1, r2a, second_a), (half, r1b, nx - 1, r2b, second_b)
    ):
        for copy in later:
            copy.wait_recv()
        for r, c in tiles():
            here = (pl.ds(r, tile_r), pl.ds(c, tile_c))
            total = gv[own_rows(y, x, r), pl.ds(base + c, tile_c)].astype(jnp.float32)
            for i in range(first_n):
                total = total + first[(i, 0) + here].astype(jnp.float32)
            for i in range(len(later)):
                total = total + second[(i,) + here].astype(jnp.float32)
            sv[pl.ds(r, tile_r), pl.ds(base + c, tile_c)] = total
            square = total * total
            for a in range(0, tile_r, 8):
                for b in range(0, tile_c, 128):
                    squares = squares + square[a:a + 8, b:b + 128]

    d_own[...] = squares
    over_dp = [
        send(d_own, d_in.at[i - 1], {"dp": lax.rem(me + i, n_dp)}) for i in range(1, n_dp)
    ]
    for i, copy in enumerate(over_dp):
        copy.wait_recv()
        squares = squares + d_in[i]
    h_own[...] = squares
    over_sh = [
        send(h_own, h_in.at[i - 1], {"shard": lax.rem(sh + i, n_sh)}) for i in range(1, n_sh)
    ]
    for copy in state_in:
        copy.wait()
    for i, copy in enumerate(over_sh):
        copy.wait_recv()
        squares = squares + h_in[i]
    square_sum = jnp.sum(jnp.sum(squares, axis=0, keepdims=True), axis=1, keepdims=True)
    limit = 0.5 * math.sqrt(entries)
    factor = jnp.minimum(1.0, limit / jnp.sqrt(square_sum + 1e-06))

    def update(base):
        for r, c in tiles():
            here = (pl.ds(r, tile_r), pl.ds(base + c, tile_c))
            clipped = factor * sv[here]
            new_first = 0.9 * mv[here] + 0.1 * clipped
            new_second = 0.95 * vv[here] + 0.05 * clipped * clipped
            master = wv[here]
            new_master = master - 0.01 * (
                (new_first * (1.0 / first_bias))
                / (jnp.sqrt(new_second * (1.0 / second_bias)) + 1e-08)
                + 0.1 * master
            )
            pv[here] = new_master.astype(jnp.bfloat16)
            wv[here] = new_master
            mv[here] = new_first
            vv[here] = new_second

    mine = block(y, x)
    update(0)
    gather_a = [
        send(pv.at[:, cols_a], fa.at[j - 1], {"dp": y * nx + at_x(j)}) for j in range(1, nx)
    ]
    direct = [
        send(pv.at[:, cols_a], out_p.at[mine, cols_a], {"dp": at_y(k) * nx + x})
        for k in range(1, ny)
    ]
    update(half)
    gather_b = [
        send(pv.at[:, cols_b], fb.at[k - 1], {"dp": at_y(k) * nx + x}) for k in range(1, ny)
    ]
    direct += [
        send(pv.at[:, cols_b], out_p.at[mine, cols_b], {"dp": y * nx + at_x(j)})
        for j in range(1, nx)
    ]
    outs = [local(pv, out_p.at[mine]), local(wv, out_w), local(mv, out_m), local(vv, out_v)]
    for j in range(1, nx):
        gather_a[j - 1].wait_recv()
        owner = block(y, lax.rem(x - j + nx, nx))
        for k in range(1, ny):
            direct.append(
                send(fa.at[j - 1], out_p.at[owner, cols_a], {"dp": at_y(k) * nx + x})
            )
        outs.append(local(fa.at[j - 1], out_p.at[owner, cols_a]))
    for k in range(1, ny):
        gather_b[k - 1].wait_recv()
        owner = block(lax.rem(y - k + ny, ny), x)
        for j in range(1, nx):
            direct.append(
                send(fb.at[k - 1], out_p.at[owner, cols_b], {"dp": y * nx + at_x(j)})
            )
        outs.append(local(fb.at[k - 1], out_p.at[owner, cols_b]))
    for copy in outs:
        copy.wait()
    for copy in direct:
        copy.wait_recv()
    for copy in started:
        copy.wait_send()


def solution(mesh):
    n_dp, n_sh = mesh.shape["dp"], mesh.shape["shard"]
    ny, nx = grid_of(n_dp)

    def per_device(gradients, master_weights, first_moment, second_moment):
        rows, width = master_weights.shape
        half = width // 2
        f32, bf16 = jnp.float32, jnp.bfloat16
        state = pltpu.VMEM((rows, width), f32)
        copies = copies_of(ny, nx, n_sh)
        hbm = pl.BlockSpec(memory_space=pltpu.HBM)
        return tuple(pl.pallas_call(
            functools.partial(step_kernel, ny, nx, n_sh, rows * n_dp * n_sh * width),
            out_shape=(
                jax.ShapeDtypeStruct((n_dp * rows, width), bf16),
                jax.ShapeDtypeStruct((rows, width), f32),
                jax.ShapeDtypeStruct((rows, width), f32),
                jax.ShapeDtypeStruct((rows, width), f32),
            ),
            in_specs=[hbm] * 4,
            out_specs=(hbm,) * 4,
            scratch_shapes=[
                pltpu.VMEM((n_dp * rows, width), bf16),
                state, state, state, state,
                pltpu.VMEM((rows, width), bf16),
                pltpu.VMEM((max(ny - 1, 1), nx, rows, half), bf16),
                pltpu.VMEM((max(nx - 1, 1), ny, rows, half), bf16),
                pltpu.VMEM((max(nx - 1, 1), rows, half), bf16),
                pltpu.VMEM((max(ny - 1, 1), rows, half), bf16),
                pltpu.VMEM((max(nx - 1, 1), rows, half), bf16),
                pltpu.VMEM((max(ny - 1, 1), rows, half), bf16),
                pltpu.VMEM((max(nx - 1, 1), rows, half), bf16),
                pltpu.VMEM((max(ny - 1, 1), rows, half), bf16),
                pltpu.VMEM((8, 128), f32),
                pltpu.VMEM((max(n_dp - 1, 1), 8, 128), f32),
                pltpu.VMEM((8, 128), f32),
                pltpu.VMEM((max(n_sh - 1, 1), 8, 128), f32),
                pltpu.SemaphoreType.DMA((8 + ny + nx,)),
                pltpu.SemaphoreType.DMA((copies,)),
                pltpu.SemaphoreType.DMA((copies,)),
            ],
            compiler_params=pltpu.CompilerParams(collective_id=0, has_side_effects=True),
        )(gradients, master_weights, first_moment, second_moment))

    in_specs = (
        P("dp", "shard", None),
        P(("shard", "dp"), None),
        P(("shard", "dp"), None),
        P(("shard", "dp"), None),
    )
    out_specs = (
        P("shard", None),
        P(("shard", "dp"), None),
        P(("shard", "dp"), None),
        P(("shard", "dp"), None),
    )
    return jax.shard_map(
        per_device, mesh=mesh, in_specs=in_specs, out_specs=out_specs, check_vma=False
    )
```

```python
import functools
import math

import jax
import jax.numpy as jnp
from jax import lax
from jax.experimental import pallas as pl
from jax.experimental.pallas import tpu as pltpu
from jax.sharding import PartitionSpec as P

MESH = pl.DeviceIdType.MESH
CHUNKS = 2
first_bias = 1.0 - math.exp(100.0 * math.log(0.9))
second_bias = 1.0 - math.exp(100.0 * math.log(0.95))


def grid_of(n_dp):
    ny = max(d for d in range(1, math.isqrt(n_dp) + 1) if n_dp % d == 0)
    return ny, n_dp // ny


def copies_of(ny, nx, n_sh):
    moves = 3 * (ny * nx - 1) * 2 * CHUNKS
    scalars = ny * nx * n_sh if ny * nx * n_sh <= 64 else ny * nx + n_sh
    return moves + scalars


def step_kernel(
    ny, nx, n_sh, entries,
    g, w, m, v,
    out_p, wv, mv, vv,
    gv, sv,
    r1a, r1b, s2a, s2b, r2a, r2b,
    d_own, d_in, h_own, met,
    lsem, ssem, rsem,
):
    n_dp = ny * nx
    rows, width = w.shape
    half = width // 2
    tile_r = 16 if rows % 16 == 0 else rows
    tile_c = min(512, half // CHUNKS)
    me = lax.axis_index("dp")
    sh = lax.axis_index("shard")
    y, x = me // nx, lax.rem(me, nx)
    count = [0]
    local_count = [0]
    started = []

    def at_y(k):
        return lax.rem(y + k, ny)

    def at_x(j):
        return lax.rem(x + j, nx)

    def block(by, bx):
        return pl.ds(pl.multiple_of((by * nx + bx) * rows, rows), rows)

    def send(src, dst, target):
        i = count[0]
        count[0] += 1
        copy = pltpu.make_async_remote_copy(
            src_ref=src, dst_ref=dst, send_sem=ssem.at[i], recv_sem=rsem.at[i],
            device_id=target, device_id_type=MESH,
        )
        copy.start()
        started.append(copy)
        return copy

    def local(src, dst):
        i = local_count[0]
        local_count[0] += 1
        copy = pltpu.make_async_copy(src, dst, lsem.at[i])
        copy.start()
        return copy

    barrier = pltpu.get_barrier_semaphore()
    for i in range(1, n_dp):
        pl.semaphore_signal(
            barrier, inc=1, device_id={"dp": lax.rem(me + i, n_dp)}, device_id_type=MESH
        )
    for i in range(1, n_sh):
        pl.semaphore_signal(
            barrier, inc=1, device_id={"shard": lax.rem(sh + i, n_sh)}, device_id_type=MESH
        )
    gap = half // CHUNKS
    order = [(at_y(k), at_x(j)) for k in range(1, ny) for j in range(1, nx)]
    order += [(at_y(k), x) for k in range(1, ny)] + [(y, at_x(j)) for j in range(1, nx)]
    grads_in = [local(g.at[0, block(*b)], gv.at[block(*b)]) for b in order + [(y, x)]]
    pl.semaphore_wait(barrier, n_dp - 1 + n_sh - 1)
    for i in range(1, n_sh):
        pl.semaphore_signal(
            met, inc=1, device_id={"shard": lax.rem(sh + i, n_sh)}, device_id_type=MESH
        )

    def cols(base, c):
        return pl.ds(base + c * gap, gap)

    def tiles():
        for r in range(0, rows, tile_r):
            for c in range(0, gap, tile_c):
                yield r, c

    def own_rows(by, bx, r):
        start = pl.multiple_of((by * nx + bx) * rows + r, tile_r)
        return pl.ds(start, tile_r)

    def first_sends(relayed):
        for c in range(CHUNKS):
            for j in (range(1, nx) if relayed else (0,)):
                for k in range(1, ny):
                    first_a[k, j, c] = send(
                        gv.at[block(at_y(k), at_x(j)), cols(0, c)],
                        r1a.at[k - 1, j, :, cols(0, c)], {"dp": at_y(k) * nx + x},
                    )
            for k in (range(1, ny) if relayed else (0,)):
                for j in range(1, nx):
                    first_b[j, k, c] = send(
                        gv.at[block(at_y(k), at_x(j)), cols(half, c)],
                        r1b.at[j - 1, k, :, cols(0, c)], {"dp": y * nx + at_x(j)},
                    )

    first_a, first_b = {}, {}
    relayed = (ny - 1) * (nx - 1)
    for copy in grads_in[:relayed]:
        copy.wait()
    first_sends(True)
    for copy in grads_in[relayed:]:
        copy.wait()
    first_sends(False)
    state_in = [local(w, wv), local(m, mv), local(v, vv)]

    second_a, second_b = {}, {}
    for chunk in range(CHUNKS):
        for j in range(1, nx):
            for k in range(1, ny):
                first_a[k, j, chunk].wait_recv()
            for r, c in tiles():
                here = (pl.ds(r, tile_r), pl.ds(chunk * gap + c, tile_c))
                part = gv[(own_rows(y, at_x(j), r),) + here[1:]].astype(jnp.float32)
                for k in range(1, ny):
                    part = part + r1a[(k - 1, j) + here].astype(jnp.float32)
                s2a[(j - 1,) + here] = part.astype(jnp.bfloat16)
            piece = (j - 1, slice(None), cols(0, chunk))
            second_a[j, chunk] = send(s2a.at[piece], r2a.at[piece], {"dp": y * nx + at_x(j)})
        for k in range(1, ny):
            for j in range(1, nx):
                first_b[j, k, chunk].wait_recv()
            for r, c in tiles():
                here = (pl.ds(r, tile_r), pl.ds(chunk * gap + c, tile_c))
                part = gv[
                    own_rows(at_y(k), x, r), pl.ds(half + chunk * gap + c, tile_c)
                ].astype(jnp.float32)
                for j in range(1, nx):
                    part = part + r1b[(j - 1, k) + here].astype(jnp.float32)
                s2b[(k - 1,) + here] = part.astype(jnp.bfloat16)
            piece = (k - 1, slice(None), cols(0, chunk))
            second_b[k, chunk] = send(s2b.at[piece], r2b.at[piece], {"dp": at_y(k) * nx + x})

    squares = jnp.zeros((8, 128), jnp.float32)
    for chunk in range(CHUNKS):
        for base, first, first_n, second, second_n, early, late in (
            (0, r1a, ny, r2a, nx, first_a, second_a), (half, r1b, nx, r2b, ny, first_b, second_b)
        ):
            for i in range(1, first_n):
                early[i, 0, chunk].wait_recv()
            for i in range(1, second_n):
                late[i, chunk].wait_recv()
            for r, c in tiles():
                here = (pl.ds(r, tile_r), pl.ds(chunk * gap + c, tile_c))
                there = pl.ds(base + chunk * gap + c, tile_c)
                total = gv[own_rows(y, x, r), there].astype(jnp.float32)
                for i in range(1, first_n):
                    total = total + first[(i - 1, 0) + here].astype(jnp.float32)
                for i in range(1, second_n):
                    total = total + second[(i - 1,) + here].astype(jnp.float32)
                sv[pl.ds(r, tile_r), there] = total
                square = total * total
                for a in range(0, tile_r, 8):
                    for b in range(0, tile_c, 128):
                        squares = squares + square[a:a + 8, b:b + 128]

    pl.semaphore_wait(met, n_sh - 1)
    squares = jnp.sum(squares, axis=0, keepdims=True)
    d_own[...] = squares
    if n_dp * n_sh <= 64:
        exchanged = [
            send(d_own, d_in.at[s * n_dp + d - 1],
                 {"dp": lax.rem(me + d, n_dp), "shard": lax.rem(sh + s, n_sh)})
            for s in reversed(range(n_sh)) for d in reversed(range(n_dp)) if s or d
        ]
        for copy in state_in:
            copy.wait()
        for copy in reversed(exchanged):
            copy.wait_recv()
        squares = squares + jnp.sum(d_in[...], axis=0)
    else:
        over_dp = [
            send(d_own, d_in.at[i - 1], {"dp": lax.rem(me + i, n_dp)}) for i in range(1, n_dp)
        ]
        for i, copy in enumerate(over_dp):
            copy.wait_recv()
            squares = squares + d_in[i]
        h_own[...] = squares
        over_sh = [
            send(h_own, d_in.at[n_dp + i - 1], {"shard": lax.rem(sh + i, n_sh)})
            for i in range(1, n_sh)
        ]
        for copy in state_in:
            copy.wait()
        for i, copy in enumerate(over_sh):
            copy.wait_recv()
            squares = squares + d_in[n_dp + i]
    square_sum = jnp.sum(squares, axis=1, keepdims=True)
    limit = 0.5 * math.sqrt(entries)
    factor = jnp.minimum(1.0, limit / jnp.sqrt(square_sum + 1e-06))

    def update(base):
        for r, c in tiles():
            here = (pl.ds(r, tile_r), pl.ds(base + c, tile_c))
            clipped = factor * sv[here]
            new_first = 0.9 * mv[here] + 0.1 * clipped
            new_second = 0.95 * vv[here] + 0.05 * clipped * clipped
            master = wv[here]
            new_master = master - 0.01 * (
                (new_first * (1.0 / first_bias))
                / (jnp.sqrt(new_second * (1.0 / second_bias)) + 1e-08)
                + 0.1 * master
            )
            out_p[own_rows(y, x, r), pl.ds(base + c, tile_c)] = new_master.astype(jnp.bfloat16)
            wv[here] = new_master
            mv[here] = new_first
            vv[here] = new_second

    def spread(owner, where, target):
        return send(out_p.at[owner, where], out_p.at[owner, where], target)

    mine = block(y, x)
    gather_a, gather_b, last = {}, {}, []
    for c in range(CHUNKS):
        update(c * gap)
        for j in range(1, nx):
            gather_a[j, c] = spread(mine, cols(0, c), {"dp": y * nx + at_x(j)})
        update(half + c * gap)
        for k in range(1, ny):
            gather_b[k, c] = spread(mine, cols(half, c), {"dp": at_y(k) * nx + x})
    for c in range(CHUNKS):
        last += [spread(mine, cols(0, c), {"dp": at_y(k) * nx + x}) for k in range(1, ny)]
        last += [spread(mine, cols(half, c), {"dp": y * nx + at_x(j)}) for j in range(1, nx)]
    for c in range(CHUNKS):
        for j in range(1, nx):
            gather_a[j, c].wait_recv()
            owner = block(y, lax.rem(x - j + nx, nx))
            last += [spread(owner, cols(0, c), {"dp": at_y(k) * nx + x}) for k in range(1, ny)]
        for k in range(1, ny):
            gather_b[k, c].wait_recv()
            owner = block(lax.rem(y - k + ny, ny), x)
            last += [spread(owner, cols(half, c), {"dp": y * nx + at_x(j)}) for j in range(1, nx)]
    for copy in last:
        copy.wait_recv()
    for copy in started:
        copy.wait_send()


def write_kernel(*refs):
    n = (len(refs) - 1) // 2
    sems = refs[-1]
    copies = [pltpu.make_async_copy(refs[i], refs[n + i], sems.at[i]) for i in range(n)]
    for copy in copies:
        copy.start()
    for copy in copies:
        copy.wait()


def write_out(arrays):
    n = len(arrays)
    size = sum(a.size * a.dtype.itemsize for a in arrays)
    return tuple(pl.pallas_call(
        write_kernel,
        out_shape=tuple(jax.ShapeDtypeStruct(a.shape, a.dtype) for a in arrays),
        in_specs=[pl.BlockSpec(memory_space=pltpu.VMEM)] * n,
        out_specs=(pl.BlockSpec(memory_space=pltpu.HBM),) * n,
        scratch_shapes=[pltpu.SemaphoreType.DMA((n,))],
        compiler_params=pltpu.CompilerParams(vmem_limit_bytes=2 * size + 2**20),
    )(*arrays))


def solution(mesh):
    n_dp, n_sh = mesh.shape["dp"], mesh.shape["shard"]
    ny, nx = grid_of(n_dp)

    def per_device(gradients, master_weights, first_moment, second_moment):
        rows, width = master_weights.shape
        half = width // 2
        f32, bf16 = jnp.float32, jnp.bfloat16
        copies = copies_of(ny, nx, n_sh)
        scalars = n_dp * n_sh - 1 if n_dp * n_sh <= 64 else n_dp + n_sh
        vmem = 24 * (n_dp + 4) * rows * width
        hbm = pl.BlockSpec(memory_space=pltpu.HBM)
        inputs = [
            pltpu.with_memory_space_constraint(a, pltpu.HBM)
            for a in (gradients, master_weights, first_moment, second_moment)
        ]
        return write_out(pl.pallas_call(
            functools.partial(step_kernel, ny, nx, n_sh, rows * n_dp * n_sh * width),
            out_shape=(
                jax.ShapeDtypeStruct((n_dp * rows, width), bf16),
                jax.ShapeDtypeStruct((rows, width), f32),
                jax.ShapeDtypeStruct((rows, width), f32),
                jax.ShapeDtypeStruct((rows, width), f32),
            ),
            in_specs=[hbm] * 4,
            out_specs=(pl.BlockSpec(memory_space=pltpu.VMEM),) * 4,
            scratch_shapes=[
                pltpu.VMEM((n_dp * rows, width), bf16),
                pltpu.VMEM((rows, width), f32),
                pltpu.VMEM((max(ny - 1, 1), nx, rows, half), bf16),
                pltpu.VMEM((max(nx - 1, 1), ny, rows, half), bf16),
                pltpu.VMEM((max(nx - 1, 1), rows, half), bf16),
                pltpu.VMEM((max(ny - 1, 1), rows, half), bf16),
                pltpu.VMEM((max(nx - 1, 1), rows, half), bf16),
                pltpu.VMEM((max(ny - 1, 1), rows, half), bf16),
                pltpu.VMEM((1, 128), f32),
                pltpu.VMEM((scalars, 1, 128), f32),
                pltpu.VMEM((1, 128), f32),
                pltpu.SemaphoreType.REGULAR,
                pltpu.SemaphoreType.DMA((n_dp + 3,)),
                pltpu.SemaphoreType.DMA((copies,)),
                pltpu.SemaphoreType.DMA((copies,)),
            ],
            compiler_params=pltpu.CompilerParams(
                collective_id=0, has_side_effects=True, vmem_limit_bytes=vmem
            ),
        )(*inputs))

    in_specs = (
        P("dp", "shard", None),
        P(("shard", "dp"), None),
        P(("shard", "dp"), None),
        P(("shard", "dp"), None),
    )
    out_specs = (
        P("shard", None),
        P(("shard", "dp"), None),
        P(("shard", "dp"), None),
        P(("shard", "dp"), None),
    )
    return jax.shard_map(
        per_device, mesh=mesh, in_specs=in_specs, out_specs=out_specs, check_vma=False
    )
```

```python
import functools
import math

import jax
import jax.numpy as jnp
from jax import lax
from jax.experimental import pallas as pl
from jax.experimental.pallas import tpu as pltpu
from jax.sharding import PartitionSpec as P

MESH = pl.DeviceIdType.MESH
CHUNKS = 2
first_bias = 1.0 - math.exp(100.0 * math.log(0.9))
second_bias = 1.0 - math.exp(100.0 * math.log(0.95))


def grid_of(n_dp):
    ny = max(d for d in range(1, math.isqrt(n_dp) + 1) if n_dp % d == 0)
    return ny, n_dp // ny


def copies_of(ny, nx, n_sh):
    moves = 3 * (ny * nx - 1) * 2 * CHUNKS
    scalars = ny * nx * n_sh if ny * nx * n_sh <= 64 else ny * nx + n_sh
    return moves + scalars


def step_kernel(
    ny, nx, n_sh, entries,
    g, w, m, v,
    out_p, wv, mv, vv,
    gv, sv,
    r1a, r1b, s2a, s2b, r2a, r2b,
    d_own, d_in, h_own, met,
    lsem, ssem, rsem,
):
    n_dp = ny * nx
    rows, width = w.shape
    half = width // 2
    tile_r = 16 if rows % 16 == 0 else rows
    tile_c = min(512, half // CHUNKS)
    me = lax.axis_index("dp")
    sh = lax.axis_index("shard")
    y, x = me // nx, lax.rem(me, nx)
    count = [0]
    local_count = [0]
    started = []

    def at_y(k):
        return lax.rem(y + k, ny)

    def at_x(j):
        return lax.rem(x + j, nx)

    def block(by, bx):
        return pl.ds(pl.multiple_of((by * nx + bx) * rows, rows), rows)

    def send(src, dst, target):
        i = count[0]
        count[0] += 1
        copy = pltpu.make_async_remote_copy(
            src_ref=src, dst_ref=dst, send_sem=ssem.at[i], recv_sem=rsem.at[i],
            device_id=target, device_id_type=MESH,
        )
        copy.start()
        started.append(copy)
        return copy

    def local(src, dst):
        i = local_count[0]
        local_count[0] += 1
        copy = pltpu.make_async_copy(src, dst, lsem.at[i])
        copy.start()
        return copy

    barrier = pltpu.get_barrier_semaphore()
    for i in range(1, n_dp):
        pl.semaphore_signal(
            barrier, inc=1, device_id={"dp": lax.rem(me + i, n_dp)}, device_id_type=MESH
        )
    for i in range(1, n_sh):
        pl.semaphore_signal(
            barrier, inc=1, device_id={"shard": lax.rem(sh + i, n_sh)}, device_id_type=MESH
        )
    gap = half // CHUNKS
    order = [(at_y(k), at_x(j)) for k in range(1, ny) for j in range(1, nx)]
    order += [(at_y(k), x) for k in range(1, ny)] + [(y, at_x(j)) for j in range(1, nx)]
    grads_in = [local(g.at[0, block(*b)], gv.at[block(*b)]) for b in order + [(y, x)]]
    pl.semaphore_wait(barrier, n_dp - 1 + n_sh - 1)
    for i in range(1, n_sh):
        pl.semaphore_signal(
            met, inc=1, device_id={"shard": lax.rem(sh + i, n_sh)}, device_id_type=MESH
        )

    def cols(base, c):
        return pl.ds(base + c * gap, gap)

    def tiles():
        for r in range(0, rows, tile_r):
            for c in range(0, gap, tile_c):
                yield r, c

    def own_rows(by, bx, r):
        start = pl.multiple_of((by * nx + bx) * rows + r, tile_r)
        return pl.ds(start, tile_r)

    def first_sends(relayed):
        for c in range(CHUNKS):
            for j in (range(1, nx) if relayed else (0,)):
                for k in range(1, ny):
                    first_a[k, j, c] = send(
                        gv.at[block(at_y(k), at_x(j)), cols(0, c)],
                        r1a.at[k - 1, j, :, cols(0, c)], {"dp": at_y(k) * nx + x},
                    )
            for k in (range(1, ny) if relayed else (0,)):
                for j in range(1, nx):
                    first_b[j, k, c] = send(
                        gv.at[block(at_y(k), at_x(j)), cols(half, c)],
                        r1b.at[j - 1, k, :, cols(0, c)], {"dp": y * nx + at_x(j)},
                    )

    first_a, first_b = {}, {}
    relayed = (ny - 1) * (nx - 1)
    for copy in grads_in[:relayed]:
        copy.wait()
    first_sends(True)
    for copy in grads_in[relayed:]:
        copy.wait()
    first_sends(False)
    state_in = [local(w, wv), local(m, mv), local(v, vv)]

    second_a, second_b = {}, {}
    for chunk in range(CHUNKS):
        for j in range(1, nx):
            for k in range(1, ny):
                first_a[k, j, chunk].wait_recv()
            for r, c in tiles():
                here = (pl.ds(r, tile_r), pl.ds(chunk * gap + c, tile_c))
                part = gv[(own_rows(y, at_x(j), r),) + here[1:]].astype(jnp.float32)
                for k in range(1, ny):
                    part = part + r1a[(k - 1, j) + here].astype(jnp.float32)
                s2a[(j - 1,) + here] = part.astype(jnp.bfloat16)
            piece = (j - 1, slice(None), cols(0, chunk))
            second_a[j, chunk] = send(s2a.at[piece], r2a.at[piece], {"dp": y * nx + at_x(j)})
        for k in range(1, ny):
            for j in range(1, nx):
                first_b[j, k, chunk].wait_recv()
            for r, c in tiles():
                here = (pl.ds(r, tile_r), pl.ds(chunk * gap + c, tile_c))
                part = gv[
                    own_rows(at_y(k), x, r), pl.ds(half + chunk * gap + c, tile_c)
                ].astype(jnp.float32)
                for j in range(1, nx):
                    part = part + r1b[(j - 1, k) + here].astype(jnp.float32)
                s2b[(k - 1,) + here] = part.astype(jnp.bfloat16)
            piece = (k - 1, slice(None), cols(0, chunk))
            second_b[k, chunk] = send(s2b.at[piece], r2b.at[piece], {"dp": at_y(k) * nx + x})

    squares = jnp.zeros((8, 128), jnp.float32)
    for chunk in range(CHUNKS):
        for base, first, first_n, second, second_n, early, late in (
            (0, r1a, ny, r2a, nx, first_a, second_a), (half, r1b, nx, r2b, ny, first_b, second_b)
        ):
            for i in range(1, first_n):
                early[i, 0, chunk].wait_recv()
            for i in range(1, second_n):
                late[i, chunk].wait_recv()
            for r, c in tiles():
                here = (pl.ds(r, tile_r), pl.ds(chunk * gap + c, tile_c))
                there = pl.ds(base + chunk * gap + c, tile_c)
                total = gv[own_rows(y, x, r), there].astype(jnp.float32)
                for i in range(1, first_n):
                    total = total + first[(i - 1, 0) + here].astype(jnp.float32)
                for i in range(1, second_n):
                    total = total + second[(i - 1,) + here].astype(jnp.float32)
                sv[pl.ds(r, tile_r), there] = total
                square = total * total
                for a in range(0, tile_r, 8):
                    for b in range(0, tile_c, 128):
                        squares = squares + square[a:a + 8, b:b + 128]

    def decay():
        for copy in state_in:
            copy.wait()
        for base in range(0, width, gap):
            for r, c in tiles():
                here = (pl.ds(r, tile_r), pl.ds(base + c, tile_c))
                mv[here] = 0.9 * mv[here]
                vv[here] = 0.95 * vv[here]

    pl.semaphore_wait(met, n_sh - 1)
    squares = jnp.sum(squares, axis=0, keepdims=True)
    d_own[...] = squares
    if n_dp * n_sh <= 64:
        exchanged = [
            send(d_own, d_in.at[s * n_dp + d - 1],
                 {"dp": lax.rem(me + d, n_dp), "shard": lax.rem(sh + s, n_sh)})
            for s in reversed(range(n_sh)) for d in reversed(range(n_dp)) if s or d
        ]
        decay()
        for copy in reversed(exchanged):
            copy.wait_recv()
        squares = squares + jnp.sum(d_in[...], axis=0)
    else:
        over_dp = [
            send(d_own, d_in.at[i - 1], {"dp": lax.rem(me + i, n_dp)}) for i in range(1, n_dp)
        ]
        for i, copy in enumerate(over_dp):
            copy.wait_recv()
            squares = squares + d_in[i]
        h_own[...] = squares
        over_sh = [
            send(h_own, d_in.at[n_dp + i - 1], {"shard": lax.rem(sh + i, n_sh)})
            for i in range(1, n_sh)
        ]
        decay()
        for i, copy in enumerate(over_sh):
            copy.wait_recv()
            squares = squares + d_in[n_dp + i]
    square_sum = jnp.sum(squares, axis=1, keepdims=True)
    limit = 0.5 * math.sqrt(entries)
    factor = jnp.minimum(1.0, limit / jnp.sqrt(square_sum + 1e-06))

    def update(base):
        for r, c in tiles():
            here = (pl.ds(r, tile_r), pl.ds(base + c, tile_c))
            clipped = factor * sv[here]
            new_first = mv[here] + 0.1 * clipped
            new_second = vv[here] + 0.05 * clipped * clipped
            master = wv[here]
            new_master = master - 0.01 * (
                (new_first * (1.0 / first_bias))
                / (jnp.sqrt(new_second * (1.0 / second_bias)) + 1e-08)
                + 0.1 * master
            )
            out_p[own_rows(y, x, r), pl.ds(base + c, tile_c)] = new_master.astype(jnp.bfloat16)
            wv[here] = new_master
            mv[here] = new_first
            vv[here] = new_second

    def spread(owner, where, target):
        return send(out_p.at[owner, where], out_p.at[owner, where], target)

    mine = block(y, x)
    gather_a, gather_b, last = {}, {}, []
    for c in range(CHUNKS):
        update(c * gap)
        for j in range(1, nx):
            gather_a[j, c] = spread(mine, cols(0, c), {"dp": y * nx + at_x(j)})
        update(half + c * gap)
        for k in range(1, ny):
            gather_b[k, c] = spread(mine, cols(half, c), {"dp": at_y(k) * nx + x})
    for c in range(CHUNKS):
        last += [spread(mine, cols(0, c), {"dp": at_y(k) * nx + x}) for k in range(1, ny)]
        last += [spread(mine, cols(half, c), {"dp": y * nx + at_x(j)}) for j in range(1, nx)]
    for c in range(CHUNKS):
        for j in range(1, nx):
            gather_a[j, c].wait_recv()
            owner = block(y, lax.rem(x - j + nx, nx))
            last += [spread(owner, cols(0, c), {"dp": at_y(k) * nx + x}) for k in range(1, ny)]
        for k in range(1, ny):
            gather_b[k, c].wait_recv()
            owner = block(lax.rem(y - k + ny, ny), x)
            last += [spread(owner, cols(half, c), {"dp": y * nx + at_x(j)}) for j in range(1, nx)]
    for copy in last:
        copy.wait_recv()
    for copy in started:
        copy.wait_send()


def write_kernel(*refs):
    n = (len(refs) - 1) // 2
    sems = refs[-1]
    copies = [pltpu.make_async_copy(refs[i], refs[n + i], sems.at[i]) for i in range(n)]
    for copy in copies:
        copy.start()
    for copy in copies:
        copy.wait()


def write_out(arrays):
    n = len(arrays)
    size = sum(a.size * a.dtype.itemsize for a in arrays)
    return tuple(pl.pallas_call(
        write_kernel,
        out_shape=tuple(jax.ShapeDtypeStruct(a.shape, a.dtype) for a in arrays),
        in_specs=[pl.BlockSpec(memory_space=pltpu.VMEM)] * n,
        out_specs=(pl.BlockSpec(memory_space=pltpu.HBM),) * n,
        scratch_shapes=[pltpu.SemaphoreType.DMA((n,))],
        compiler_params=pltpu.CompilerParams(vmem_limit_bytes=2 * size + 2**20),
    )(*arrays))


def solution(mesh):
    n_dp, n_sh = mesh.shape["dp"], mesh.shape["shard"]
    ny, nx = grid_of(n_dp)

    def per_device(gradients, master_weights, first_moment, second_moment):
        rows, width = master_weights.shape
        half = width // 2
        f32, bf16 = jnp.float32, jnp.bfloat16
        copies = copies_of(ny, nx, n_sh)
        scalars = n_dp * n_sh - 1 if n_dp * n_sh <= 64 else n_dp + n_sh
        vmem = 24 * (n_dp + 4) * rows * width
        hbm = pl.BlockSpec(memory_space=pltpu.HBM)
        inputs = [
            pltpu.with_memory_space_constraint(a, pltpu.HBM)
            for a in (gradients, master_weights, first_moment, second_moment)
        ]
        return write_out(pl.pallas_call(
            functools.partial(step_kernel, ny, nx, n_sh, rows * n_dp * n_sh * width),
            out_shape=(
                jax.ShapeDtypeStruct((n_dp * rows, width), bf16),
                jax.ShapeDtypeStruct((rows, width), f32),
                jax.ShapeDtypeStruct((rows, width), f32),
                jax.ShapeDtypeStruct((rows, width), f32),
            ),
            in_specs=[hbm] * 4,
            out_specs=(pl.BlockSpec(memory_space=pltpu.VMEM),) * 4,
            scratch_shapes=[
                pltpu.VMEM((n_dp * rows, width), bf16),
                pltpu.VMEM((rows, width), f32),
                pltpu.VMEM((max(ny - 1, 1), nx, rows, half), bf16),
                pltpu.VMEM((max(nx - 1, 1), ny, rows, half), bf16),
                pltpu.VMEM((max(nx - 1, 1), rows, half), bf16),
                pltpu.VMEM((max(ny - 1, 1), rows, half), bf16),
                pltpu.VMEM((max(nx - 1, 1), rows, half), bf16),
                pltpu.VMEM((max(ny - 1, 1), rows, half), bf16),
                pltpu.VMEM((1, 128), f32),
                pltpu.VMEM((scalars, 1, 128), f32),
                pltpu.VMEM((1, 128), f32),
                pltpu.SemaphoreType.REGULAR,
                pltpu.SemaphoreType.DMA((n_dp + 3,)),
                pltpu.SemaphoreType.DMA((copies,)),
                pltpu.SemaphoreType.DMA((copies,)),
            ],
            compiler_params=pltpu.CompilerParams(
                collective_id=0, has_side_effects=True, vmem_limit_bytes=vmem
            ),
        )(*inputs))

    in_specs = (
        P("dp", "shard", None),
        P(("shard", "dp"), None),
        P(("shard", "dp"), None),
        P(("shard", "dp"), None),
    )
    out_specs = (
        P("shard", None),
        P(("shard", "dp"), None),
        P(("shard", "dp"), None),
        P(("shard", "dp"), None),
    )
    return jax.shard_map(
        per_device, mesh=mesh, in_specs=in_specs, out_specs=out_specs, check_vma=False
    )
```
